32 devices in a mesh: grp: 2 (over x), tile: 16 (over z, y, core).
Axes of the slice: x: 2, y: 2, z: 4, core: 2. Of those that a mesh axis runs over, the one named last changes fastest.
Arguments:
- habitat: int32 [32, 4, 512], P(('grp', 'tile')), parts along dimension 0, may hold values from 0 to 15
- table: float32 [16], replicated, may hold values from 0.25 to 2
- source_cell: int32 [512], P('grp'), parts along dimension 0, may hold values from 0 to 32767
- ground_cell: int32 [512], P('grp'), parts along dimension 0, may hold values from 0 to 32767
- start_potential: float32 [32, 4, 512, 256], P(('grp', 'tile')), parts along dimension 0, may hold values from -30 to 30
Outputs:
- potentials: float32 [32, 4, 512, 256], P(('grp', 'tile')), parts along dimension 0
- residual: float32 [32, 4, 512, 256], P(('grp', 'tile')), parts along dimension 0
- resistance: float32 [512], P('grp'), parts along dimension 0
The draws below stay inside these ranges and needn't reach their ends.
There are 2 independent parts, one for each index of `grp`. The reference program is written for one: setup_inputs(seed, part) draws one part's arguments, and reference() takes and returns one part's arrays. A program takes and returns all parts, laid end to end along the dimension named above; an argument that names none is the same for every part. Nothing has to cross between parts.
Inputs may be any that keep to these rules, and one draw needn't show every extreme that they name: `source_cell`: an index row * 1024 + column of the raster. `ground_cell`: an index row * 1024 + column of the raster.
All inputs are finite; a program needn't handle non-finite values.
Results may differ from the reference program's by a relative error of at most 0.00018.
Values sent between devices are 32-bit elements; how exact they have to be, the bound alone decides.
A program may use at most 128 MiB of HBM per device.

```python
import math
import jax
import jax.numpy as jnp

CX = 4
CY = 512
R = 256
CLASSES = 16
ITERS = 2
BLOCKS = 16
NX = 32
NY = 1024


def draw_start_potential(key, part):
    base_key = jax.random.fold_in(jax.random.fold_in(key, 17), 0)
    block_rows = jnp.arange(BLOCKS) // 2
    raster_rows = block_rows[:, None] * CX + jnp.arange(CX)[None, :]
    ramp = jnp.exp(1.1513 * raster_rows.astype(jnp.float32) / max(NX - 1, 1))
    field = jax.random.normal(base_key, (BLOCKS, CX, CY, R), jnp.float32)
    return field * ramp[:, :, None, None]


def set_ends(result, rng, low, largest):
    longest = result.shape.index(max(result.shape))
    spots = []
    for shift in (0, 1):
        where = [jax.random.randint(jax.random.fold_in(rng, axis), (), 0, length) for axis, length in enumerate(result.shape)]
        where[longest] = (where[longest] + shift) % result.shape[longest]
        spots.append(tuple(where))
    return result.at[spots[0]].set(low).at[spots[1]].set(largest)


def setup_inputs(seed: int = 0, part: int = 0) -> dict:
    keys = jax.random.split(jax.random.key(seed), 6)
    part_splits = jax.random.split(jax.random.fold_in(keys[5], part), 6)
    habitat = set_ends(jax.random.randint(part_splits[0], (BLOCKS, CX, CY), 0, CLASSES), jax.random.fold_in(part_splits[0], 1), 0, CLASSES - 1).astype(jnp.int32)
    table = jnp.clip(jnp.exp(jax.random.uniform(keys[1], (CLASSES,), jnp.float32, math.log(0.25), math.log(2.0))), 0.25, 2.0)
    source_cell = set_ends(jax.random.randint(part_splits[2], (R,), 0, NX * NY), jax.random.fold_in(part_splits[2], 1), 0, (NX * NY) - 1).astype(jnp.int32)
    ground_cell = set_ends(jax.random.randint(part_splits[3], (R,), 0, NX * NY), jax.random.fold_in(part_splits[3], 1), 0, (NX * NY) - 1).astype(jnp.int32)
    start_potential = draw_start_potential(jax.random.fold_in(jax.random.fold_in(keys[5], part), 71), part)
    return dict(habitat=habitat, table=table, source_cell=source_cell, ground_cell=ground_cell, start_potential=start_potential)


def to_raster(blocks):
    block_count, rows_here, cols_here = blocks.shape[0], blocks.shape[1], blocks.shape[2]
    trailing = blocks.shape[3:]
    blocks_grid = blocks.reshape((block_count // 2, 2, rows_here, cols_here) + trailing)
    blocks_grid = jnp.swapaxes(blocks_grid, 1, 2)
    return blocks_grid.reshape((block_count // 2 * rows_here, 2 * cols_here) + trailing)


def to_blocks(raster, rows_here, cols_here):
    trailing = raster.shape[2:]
    blocks_grid = raster.reshape((raster.shape[0] // rows_here, rows_here, 2, cols_here) + trailing)
    blocks_grid = jnp.swapaxes(blocks_grid, 1, 2)
    return blocks_grid.reshape((raster.shape[0] // rows_here * 2, rows_here, cols_here) + trailing)


def reference(habitat, table, source_cell, ground_cell, start_potential):
    classes = to_raster(habitat)
    conduct = table[classes]
    row_count, col_count = classes.shape[0], classes.shape[1]
    padded = jnp.pad(conduct, 1)
    row_index = jnp.arange(row_count)[:, None]
    col_index = jnp.arange(col_count)[None, :]
    north_w = jnp.where(row_index > 0, 0.5 * (conduct + padded[:-2, 1:-1]), 0.0)
    south_w = jnp.where(row_index < row_count - 1, 0.5 * (conduct + padded[2:, 1:-1]), 0.0)
    west_w = jnp.where(col_index > 0, 0.5 * (conduct + padded[1:-1, :-2]), 0.0)
    east_w = jnp.where(col_index < col_count - 1, 0.5 * (conduct + padded[1:-1, 2:]), 0.0)
    cell_ids = (row_index * col_count + col_index).astype(jnp.int32)
    ground_mask = (cell_ids[:, :, None] == ground_cell[None, None, :]).astype(jnp.float32)
    diagonal = (north_w + south_w + west_w + east_w)[:, :, None] + ground_mask
    source_field = (cell_ids[:, :, None] == source_cell[None, None, :]).astype(jnp.float32)

    def operate(field):
        pad_field = jnp.pad(field, ((1, 1), (1, 1), (0, 0)))
        applied = diagonal * field - north_w[:, :, None] * pad_field[:-2, 1:-1]
        applied = applied - south_w[:, :, None] * pad_field[2:, 1:-1]
        applied = applied - west_w[:, :, None] * pad_field[1:-1, :-2]
        return applied - east_w[:, :, None] * pad_field[1:-1, 2:]

    potentials = to_raster(start_potential)
    residual = source_field - operate(potentials)
    direction = residual
    norm_now = jnp.sum(residual * residual, axis=(0, 1))
    for iteration in range(ITERS):
        applied = operate(direction)
        step_size = norm_now / jnp.sum(direction * applied, axis=(0, 1))
        potentials = potentials + step_size * direction
        residual = residual - step_size * applied
        if iteration + 1 < ITERS:
            norm_next = jnp.sum(residual * residual, axis=(0, 1))
            direction = residual + (norm_next / norm_now) * direction
            norm_now = norm_next
    flattened = potentials.reshape((row_count * col_count, potentials.shape[2]))
    columns = jnp.arange(potentials.shape[2], dtype=jnp.int32)
    resistance = flattened[source_cell, columns] - flattened[ground_cell, columns]
    rows_here, cols_here = habitat.shape[1], habitat.shape[2]
    return to_blocks(potentials, rows_here, cols_here), to_blocks(residual, rows_here, cols_here), resistance
```

```python
import functools

import jax
import jax.numpy as jnp
from jax import lax
from jax.experimental import pallas as pl
from jax.experimental.pallas import tpu as pltpu
from jax.sharding import PartitionSpec as P

LANES = 128
TILE = 8
PAD = 2 * TILE
MESH = pl.DeviceIdType.MESH


def kernel(n, rows, cols, table_ref, habitat_ref, source_ref, ground_ref, start_ref,
           pot_ref, res_ref, drop_ref,
           X, R, W, U, V, H, D, C, T, TV, TH, S, O1, O2,
           load_sem, cond_send, cond_recv, side_send, side_recv,
           row_send, row_recv, relay_send, relay_recv, sum_send, sum_recv, out_sem):
    halves = X.shape[0]
    width = cols + 2 * PAD
    me = lax.axis_index("tile")
    chips = n // 2
    chip = me // 2
    core = me % 2
    odd = chip % 2
    side = me + 1 - 2 * core
    partner = me + 2 - 4 * odd
    own = pl.ds(PAD, cols)

    def load(h):
        return pltpu.make_async_copy(
            start_ref.at[0, :, :, pl.ds(h * LANES, LANES)], X.at[h, pl.ds(rows, rows), own, :],
            load_sem.at[h])

    for h in range(halves):
        load(h).start()

    barrier = pltpu.get_barrier_semaphore()

    def greet(d, _):
        pl.semaphore_signal(barrier, inc=1, device_id={"tile": (me + d) % n}, device_id_type=MESH)
        return 0

    cells = habitat_ref[0]
    cond = jnp.zeros(cells.shape, jnp.float32)
    for level in range(table_ref.shape[0]):
        cond = jnp.where(cells == level, table_ref[level], cond)
    for slot in range(5):
        C[slot] = jnp.zeros(C.shape[1:], jnp.float32)
    C[5, 0:rows, :] = cond
    C[5, rows:2 * rows, :] = cond

    def zero(ref, lead, c):
        count = ref.shape[1]
        ref[lead[0], :, c:c + TILE, :] = jnp.zeros((count, TILE, LANES), jnp.float32)

    for h in range(halves):
        for c in (0, width - TILE):
            zero(X, (h,), c)
            zero(R, (h,), c)
            zero(W, (h,), c)
        @pl.when(core == 0)
        def _():
            zero(X, (h,), TILE)
        @pl.when(core == 1)
        def _():
            zero(X, (h,), width - PAD)
        @pl.when(chip == 0)
        def _():
            X[h, 0:rows] = jnp.zeros((rows, width, LANES), jnp.float32)
        @pl.when(chip == chips - 1)
        def _():
            X[h, 2 * rows:3 * rows] = jnp.zeros((rows, width, LANES), jnp.float32)

    lax.fori_loop(1, n, greet, 0)
    pl.semaphore_wait(barrier, n - 1)

    def cond_copy(target, slot):
        return pltpu.make_async_remote_copy(
            src_ref=C.at[5], dst_ref=C.at[slot], send_sem=cond_send.at[slot],
            recv_sem=cond_recv.at[slot], device_id={"tile": target}, device_id_type=MESH)

    has_above = chip > 0
    has_below = chip < chips - 1

    def cond_each(act):
        act(cond_copy(side, 2))

        @pl.when(has_above)
        def _():
            act(cond_copy(me - 2, 1))
            act(cond_copy(side - 2, 4))

        @pl.when(has_below)
        def _():
            act(cond_copy(me + 2, 0))
            act(cond_copy(side + 2, 3))

    cond_each(lambda copy: copy.start())

    inner = pl.multiple_of(PAD + (1 - core) * (cols - TILE), TILE)

    def side_copy(h):
        dst = pl.multiple_of((1 - core) * TILE + core * (PAD + cols), TILE)
        return pltpu.make_async_remote_copy(
            src_ref=X.at[h, pl.ds(rows, rows), pl.ds(inner, TILE), :],
            dst_ref=X.at[h, pl.ds(rows, rows), pl.ds(dst, TILE), :],
            send_sem=side_send.at[h], recv_sem=side_recv.at[h],
            device_id={"tile": side}, device_id_type=MESH)

    span = pl.ds(pl.multiple_of(PAD - core * TILE, TILE), cols + TILE)

    def row_copy(h, i):
        r = (i + odd) % rows
        return pltpu.make_async_remote_copy(
            src_ref=X.at[h, rows + r, span, :], dst_ref=X.at[h, odd * 2 * rows + r, span, :],
            send_sem=row_send.at[h, i], recv_sem=row_recv.at[h, i],
            device_id={"tile": partner}, device_id_type=MESH)

    def row_wait(h, i):
        r = (i + 1 - odd) % rows
        place = X.at[h, (1 - odd) * 2 * rows + r, span, :]
        pltpu.make_async_remote_copy(
            src_ref=place, dst_ref=place, send_sem=row_send.at[h, i], recv_sem=row_recv.at[h, i],
            device_id={"tile": partner}, device_id_type=MESH).wait_recv()

    relay_to = me + 4 - 8 * odd
    can_relay = jnp.where(odd == 0, chip + 2 < chips, chip >= 2)
    gets_relay = jnp.where(odd == 0, chip >= 2, chip + 2 < chips)

    def relay_copy(h, i):
        src = (1 - odd) * (2 * rows + 1) + i
        dst = odd * 2 * rows + (1 - odd) + i
        return pltpu.make_async_remote_copy(
            src_ref=X.at[h, src, span, :], dst_ref=X.at[h, dst, span, :],
            send_sem=relay_send.at[h, i], recv_sem=relay_recv.at[h, i],
            device_id={"tile": relay_to}, device_id_type=MESH)

    def relay_wait(h):
        @pl.when(gets_relay)
        def _():
            for i in range(rows - 1):
                dst = odd * 2 * rows + (1 - odd) + i
                place = X.at[h, dst, span, :]
                pltpu.make_async_remote_copy(
                    src_ref=place, dst_ref=place, send_sem=relay_send.at[h, i],
                    recv_sem=relay_recv.at[h, i],
                    device_id={"tile": relay_to}, device_id_type=MESH).wait_recv()

    def take(h, i):
        row_wait(h, i)
        if i < rows - 1:
            @pl.when(can_relay)
            def _():
                relay_copy(h, i).start()

    for h in range(halves):
        load(h).wait()
        side_copy(h).start()
    for h in range(halves):
        side_copy(h).wait_recv()
        for i in range(rows):
            row_copy(h, i).start()

    cond_copy(side, 2).wait_recv()

    @pl.when(has_above)
    def _():
        cond_copy(me - 2, 0).wait_recv()
        cond_copy(side - 2, 3).wait_recv()

    @pl.when(has_below)
    def _():
        cond_copy(me + 2, 1).wait_recv()
        cond_copy(side + 2, 4).wait_recv()

    first = lax.broadcasted_iota(jnp.int32, (2 * rows, LANES), 0) < rows

    def turned(above, here, below, j):
        lanes = slice(j * LANES, (j + 1) * LANES)
        top = jnp.where(first, C[above, :, lanes], C[here, :, lanes])
        blank = jnp.zeros((LANES - 4 * rows, LANES), jnp.float32)
        return jnp.transpose(jnp.concatenate([top, C[below, :, lanes], blank], 0))

    for j in range(cols // LANES):
        T[PAD + j * LANES:PAD + (j + 1) * LANES, :] = turned(0, 5, 1, j)
    for c in (0, TILE, width - PAD, width - TILE):
        T[c:c + TILE, :] = jnp.zeros((TILE, LANES), jnp.float32)

    @pl.when(core == 0)
    def _():
        T[width - PAD:width - TILE, :] = turned(3, 2, 4, 0)[0:TILE]

    @pl.when(core == 1)
    def _():
        T[TILE:PAD, :] = turned(3, 2, 4, cols // LANES - 1)[LANES - TILE:]

    def global_col(c):
        return core * cols - PAD + c + lax.broadcasted_iota(jnp.int32, (TILE, LANES), 0)

    global_row = chip * rows - rows + lax.broadcasted_iota(jnp.int32, (TILE, LANES), 1)
    total_rows, total_cols = chips * rows, 2 * cols

    def edges(t, _):
        c = pl.multiple_of(t * TILE, TILE)
        here = T[pl.ds(c, TILE), :]
        east = T[pl.ds(c + 1, TILE), :]
        south = pltpu.roll(here, LANES - 1, 1)
        gc = global_col(c)
        in_row = (global_row >= 0) & (global_row < total_rows - 1)
        TV[pl.ds(c, TILE), :] = jnp.where(in_row, 0.5 * (here + south), 0.0)
        in_col = (gc >= 0) & (gc < total_cols - 1)
        TH[pl.ds(c, TILE), :] = jnp.where(in_col, 0.5 * (here + east), 0.0)
        return 0

    TH[0:TILE, :] = jnp.zeros((TILE, LANES), jnp.float32)
    H[:, 0:TILE, :] = jnp.zeros((H.shape[0], TILE, LANES), jnp.float32)
    lax.fori_loop(1, width // TILE - 1, edges, 0)

    def spread(t, _):
        c = pl.multiple_of(t * TILE, TILE)
        at = pl.ds(c, TILE)
        v = TV[at, :]
        east = TH[at, :]
        west = TH[pl.ds(c - 1, TILE), :]
        diag = v + pltpu.roll(v, 1, 1) + east + west
        shape = (TILE, LANES)
        for k in range(2 * rows + 1):
            V[k, at, :] = jnp.broadcast_to(v[:, k + 1:k + 2], shape)
        for k in range(2 * rows):
            H[k, at, :] = jnp.broadcast_to(east[:, k + 2:k + 3], shape)
            D[k, at, :] = jnp.broadcast_to(diag[:, k + 2:k + 3], shape)
        return 0

    lax.fori_loop(1, width // TILE - 1, spread, 0)

    def cell_ids(c, count, top):
        shape = (count, TILE, LANES)
        r = chip * rows + top + lax.broadcasted_iota(jnp.int32, shape, 0)
        col = core * cols - PAD + c + lax.broadcasted_iota(jnp.int32, shape, 1)
        return r * total_cols + col

    def applied(ref, h, skip, count, c, low, grounded):
        at = pl.ds(c, TILE)
        f = ref[h, skip:skip + count + 2, at, :]
        left = ref[h, skip + 1:skip + 1 + count, pl.ds(c - 1, TILE), :]
        right = ref[h, skip + 1:skip + 1 + count, pl.ds(c + 1, TILE), :]
        mid = f[1:count + 1]
        v = V[low:low + count + 1, at, :]
        out = D[low:low + count, at, :] * mid + jnp.where(grounded, mid, 0.0)
        out = out - v[:count] * f[:count] - v[1:] * f[2:]
        out = out - H[low:low + count, pl.ds(c - 1, TILE), :] * left
        return out - H[low:low + count, at, :] * right, mid

    def compute(h):
        src = source_ref[h:h + 1, :][None]
        gnd = ground_ref[h:h + 1, :][None]
        inner_rows = 2 * rows

        def pass_r(t, _):
            c = pl.multiple_of(t * TILE, TILE)
            ids = cell_ids(c, inner_rows, -2)
            a, _mid = applied(X, h, 1, inner_rows, c, 0, ids == gnd)
            R[h, :, pl.ds(c, TILE), :] = jnp.where(ids == src, 1.0, 0.0) - a
            return 0

        def pass_w(t, _):
            c = pl.multiple_of(t * TILE, TILE)
            count = inner_rows - 2
            ids = cell_ids(c, count, -1)
            a, _mid = applied(R, h, 0, count, c, 1, ids == gnd)
            W[h, :, pl.ds(c, TILE), :] = a
            return 0

        def pass_u(t, acc):
            c = pl.multiple_of(t * TILE, TILE)
            at = pl.ds(c, TILE)
            ids = cell_ids(c, rows, 0)
            is_g = ids == gnd
            u, w = applied(W, h, 0, rows, c, 2, is_g)
            U[h, :, pl.ds(c - PAD, TILE), :] = u
            r = R[h, 2:2 + rows, at, :]
            x = X[h, rows:2 * rows, at, :]
            sign = jnp.where(ids == src, 1.0, 0.0) - jnp.where(is_g, 1.0, 0.0)
            terms = (r * r, r * w, w * w, w * u, sign * x, sign * r, sign * w)
            return tuple(s + jnp.sum(term, axis=0) for s, term in zip(acc, terms))

        tiles = width // TILE
        lax.fori_loop(1, tiles - 1, pass_r, 0)
        lax.fori_loop(1, tiles - 1, pass_w, 0)
        acc = lax.fori_loop(2, tiles - 2, pass_u,
                            tuple(jnp.zeros((TILE, LANES), jnp.float32) for _ in range(7)))
        sums = [jnp.sum(s, axis=0, keepdims=True) for s in acc]
        S[h, me] = jnp.concatenate(sums + [jnp.zeros((1, LANES), jnp.float32)], 0)

    def sum_copy(h, d):
        return pltpu.make_async_remote_copy(
            src_ref=S.at[h, me], dst_ref=S.at[h, me], send_sem=sum_send.at[h, d],
            recv_sem=sum_recv.at[h, d],
            device_id={"tile": (me + d) % n}, device_id_type=MESH)

    def send_sums(h):
        lax.fori_loop(1, n, lambda d, _: (sum_copy(h, d).start(), 0)[1], 0)

    def out_copies(h):
        lanes = pl.ds(h * LANES, LANES)
        return (
            pltpu.make_async_copy(O1.at[h], pot_ref.at[0, :, :, lanes], out_sem.at[h, 0]),
            pltpu.make_async_copy(O2.at[h], res_ref.at[0, :, :, lanes], out_sem.at[h, 1]),
        )

    def finish(h):
        def arrive(d, _):
            place = S.at[h, (me + n - d) % n]
            pltpu.make_async_remote_copy(
                src_ref=place, dst_ref=place, send_sem=sum_send.at[h, d],
                recv_sem=sum_recv.at[h, d], device_id={"tile": (me + d) % n},
                device_id_type=MESH).wait_recv()
            return 0

        lax.fori_loop(1, n, arrive, 0)
        total = S[h, 0]
        for k in range(1, n):
            total = total + S[h, k]
        m0, m1, m2, m3, ex, er, ew = (total[k:k + 1] for k in range(7))
        a0 = m0 / m1
        next_norm = a0 * (a0 * m2 - m1)
        ratio = next_norm / m0
        curve = m1 - a0 * (2.0 * m2 - a0 * m3)
        a1 = next_norm / (curve - ratio * next_norm / a0)
        p = a0 + a1 * (1.0 + ratio)
        q = a1 * a0
        drop_ref[h:h + 1, :] = ex + p * er - q * ew
        p3, q3 = p[None], q[None]

        def last(t, _):
            c = pl.multiple_of(t * TILE, TILE)
            at = pl.ds(c + PAD, TILE)
            r = R[h, 2:2 + rows, at, :]
            w = W[h, 1:1 + rows, at, :]
            O1[h, :, pl.ds(c, TILE), :] = X[h, rows:2 * rows, at, :] + p3 * r - q3 * w
            O2[h, :, pl.ds(c, TILE), :] = r - p3 * w + q3 * U[h, :, pl.ds(c, TILE), :]
            return 0

        lax.fori_loop(0, cols // TILE, last, 0)
        for copy in out_copies(h):
            copy.start()

    for i in range(rows):
        take(0, i)
    relay_wait(0)
    for h in range(halves):
        compute(h)
        send_sums(h)
        if h + 1 < halves:
            for i in range(rows - 2):
                take(h + 1, i)
        finish(h)
        if h + 1 < halves:
            for i in range(rows - 2, rows):
                take(h + 1, i)
            relay_wait(h + 1)

    cond_each(lambda copy: copy.wait_send())
    for h in range(halves):
        side_copy(h).wait_send()
        for i in range(rows):
            row_copy(h, i).wait_send()

        @pl.when(can_relay)
        def _():
            for i in range(rows - 1):
                relay_copy(h, i).wait_send()

        lax.fori_loop(1, n, lambda d, _: (sum_copy(h, d).wait_send(), 0)[1], 0)
        for copy in out_copies(h):
            copy.wait()


def solution(mesh):
    n = mesh.shape["tile"]

    def shards(habitat, table, source_cell, ground_cell, start_potential):
        _, rows, cols, rhs = start_potential.shape
        halves = rhs // LANES
        width = cols + 2 * PAD
        f32 = jnp.float32
        dma = pltpu.SemaphoreType.DMA
        field = jax.ShapeDtypeStruct(start_potential.shape, f32)
        vmem = pl.BlockSpec(memory_space=pltpu.VMEM)
        hbm = pl.BlockSpec(memory_space=pltpu.HBM)
        potentials, residual, drop = pl.pallas_call(
            functools.partial(kernel, n, rows, cols),
            out_shape=(field, field, jax.ShapeDtypeStruct((halves, LANES), f32)),
            in_specs=[pl.BlockSpec(memory_space=pltpu.SMEM), vmem, vmem, vmem, hbm],
            out_specs=(hbm, hbm, vmem),
            scratch_shapes=[
                pltpu.VMEM((halves, 3 * rows, width, LANES), f32),
                pltpu.VMEM((halves, 2 * rows, width, LANES), f32),
                pltpu.VMEM((halves, 2 * rows - 2, width, LANES), f32),
                pltpu.VMEM((halves, rows, cols, LANES), f32),
                pltpu.VMEM((2 * rows + 1, width, LANES), f32),
                pltpu.VMEM((2 * rows, width, LANES), f32),
                pltpu.VMEM((2 * rows, width, LANES), f32),
                pltpu.VMEM((6, 2 * rows, cols), f32),
                pltpu.VMEM((width, LANES), f32),
                pltpu.VMEM((width, LANES), f32),
                pltpu.VMEM((width, LANES), f32),
                pltpu.VMEM((halves, n, TILE, LANES), f32),
                pltpu.VMEM((halves, rows, cols, LANES), f32),
                pltpu.VMEM((halves, rows, cols, LANES), f32),
                dma((halves,)),
                dma((5,)), dma((5,)),
                dma((halves,)), dma((halves,)),
                dma((halves, rows)), dma((halves, rows)),
                dma((halves, rows - 1)), dma((halves, rows - 1)),
                dma((halves, n)), dma((halves, n)),
                dma((halves, 2)),
            ],
            compiler_params=pltpu.CompilerParams(
                collective_id=0, has_side_effects=True, vmem_limit_bytes=48 * 2**20),
        )(table, habitat, source_cell.reshape(halves, LANES),
          ground_cell.reshape(halves, LANES), start_potential)
        return potentials, residual, drop.reshape(rhs)

    placed = (
        P(("grp", "tile"), None, None),
        P(),
        P("grp"),
        P("grp"),
        P(("grp", "tile"), None, None, None),
    )
    return jax.shard_map(
        shards,
        mesh=mesh,
        in_specs=placed,
        out_specs=(placed[4], placed[4], P("grp")),
        check_vma=False,
    )
```

```python
import functools

import jax
import jax.numpy as jnp
from jax import lax
from jax.experimental import pallas as pl
from jax.experimental.pallas import tpu as pltpu
from jax.sharding import PartitionSpec as P

LANES = 128
TILE = 8
PAD = 2 * TILE
MESH = pl.DeviceIdType.MESH


def kernel(n, rows, cols, table_ref, habitat_ref, source_ref, ground_ref, start_ref,
           pot_ref, res_ref, drop_ref,
           X, R, W, U, V, H, D, C, T, TV, TH, S,
           load_sem, cond_send, cond_recv, side_send, side_recv,
           row_send, row_recv, relay_send, relay_recv, sum_send, sum_recv):
    halves = X.shape[0]
    width = cols + 2 * PAD
    me = lax.axis_index("tile")
    chips = n // 2
    chip = me // 2
    core = me % 2
    odd = chip % 2
    side = me + 1 - 2 * core
    partner = me + 2 - 4 * odd
    own = pl.ds(PAD, cols)
    travel = cols // TILE + 1
    bounds = [0, travel * 19 // 65, travel * 37 // 65, travel * 53 // 65, travel]
    pieces = len(bounds) - 1

    def load(h):
        return pltpu.make_async_copy(
            start_ref.at[0, :, :, pl.ds(h * LANES, LANES)], X.at[h, pl.ds(rows, rows), own, :],
            load_sem.at[h])

    for h in range(halves):
        load(h).start()

    barrier = pltpu.get_barrier_semaphore()

    def greet(d, _):
        pl.semaphore_signal(barrier, inc=1, device_id={"tile": (me + d) % n}, device_id_type=MESH)
        return 0

    cells = habitat_ref[0]
    cond = jnp.zeros(cells.shape, jnp.float32)
    for level in range(table_ref.shape[0]):
        cond = jnp.where(cells == level, table_ref[level], cond)
    for slot in range(5):
        C[slot] = jnp.zeros(C.shape[1:], jnp.float32)
    C[5, 0:rows, :] = cond
    C[5, rows:2 * rows, :] = cond

    def zero(ref, lead, c):
        count = ref.shape[1]
        ref[lead[0], :, c:c + TILE, :] = jnp.zeros((count, TILE, LANES), jnp.float32)

    for h in range(halves):
        for c in (0, width - TILE):
            zero(X, (h,), c)
            zero(R, (h,), c)
            zero(W, (h,), c)
        @pl.when(core == 0)
        def _():
            zero(X, (h,), TILE)
        @pl.when(core == 1)
        def _():
            zero(X, (h,), width - PAD)
        @pl.when(chip == 0)
        def _():
            X[h, 0:rows] = jnp.zeros((rows, width, LANES), jnp.float32)
        @pl.when(chip == chips - 1)
        def _():
            X[h, 2 * rows:3 * rows] = jnp.zeros((rows, width, LANES), jnp.float32)

    lax.fori_loop(1, n, greet, 0)
    pl.semaphore_wait(barrier, n - 1)

    def cond_copy(target, slot):
        return pltpu.make_async_remote_copy(
            src_ref=C.at[5], dst_ref=C.at[slot], send_sem=cond_send.at[slot],
            recv_sem=cond_recv.at[slot], device_id={"tile": target}, device_id_type=MESH)

    has_above = chip > 0
    has_below = chip < chips - 1

    def cond_each(act):
        act(cond_copy(side, 2))

        @pl.when(has_above)
        def _():
            act(cond_copy(me - 2, 1))
            act(cond_copy(side - 2, 4))

        @pl.when(has_below)
        def _():
            act(cond_copy(me + 2, 0))
            act(cond_copy(side + 2, 3))

    cond_each(lambda copy: copy.start())

    inner = pl.multiple_of(PAD + (1 - core) * (cols - TILE), TILE)

    def side_copy(h):
        dst = pl.multiple_of((1 - core) * TILE + core * (PAD + cols), TILE)
        return pltpu.make_async_remote_copy(
            src_ref=X.at[h, pl.ds(rows, rows), pl.ds(inner, TILE), :],
            dst_ref=X.at[h, pl.ds(rows, rows), pl.ds(dst, TILE), :],
            send_sem=side_send.at[h], recv_sem=side_recv.at[h],
            device_id={"tile": side}, device_id_type=MESH)

    def span(j):
        start = pl.multiple_of(PAD - core * TILE + bounds[j] * TILE, TILE)
        return pl.ds(start, (bounds[j + 1] - bounds[j]) * TILE)

    def row_copy(h, j, i):
        r = (i + odd) % rows
        return pltpu.make_async_remote_copy(
            src_ref=X.at[h, rows + r, span(j), :],
            dst_ref=X.at[h, odd * 2 * rows + r, span(j), :],
            send_sem=row_send.at[h, j, i], recv_sem=row_recv.at[h, j, i],
            device_id={"tile": partner}, device_id_type=MESH)

    def row_wait(h, j, i):
        r = (i + 1 - odd) % rows
        place = X.at[h, (1 - odd) * 2 * rows + r, span(j), :]
        pltpu.make_async_remote_copy(
            src_ref=place, dst_ref=place,
            send_sem=row_send.at[h, j, i], recv_sem=row_recv.at[h, j, i],
            device_id={"tile": partner}, device_id_type=MESH).wait_recv()

    relay_to = me + 4 - 8 * odd
    can_relay = jnp.where(odd == 0, chip + 2 < chips, chip >= 2)
    gets_relay = jnp.where(odd == 0, chip >= 2, chip + 2 < chips)

    def relay_copy(h, j, i):
        src = (1 - odd) * (2 * rows + 1) + i
        dst = odd * 2 * rows + (1 - odd) + i
        return pltpu.make_async_remote_copy(
            src_ref=X.at[h, src, span(j), :], dst_ref=X.at[h, dst, span(j), :],
            send_sem=relay_send.at[h, j, i], recv_sem=relay_recv.at[h, j, i],
            device_id={"tile": relay_to}, device_id_type=MESH)

    def relay_wait(h, j):
        @pl.when(gets_relay)
        def _():
            for i in range(rows - 1):
                dst = odd * 2 * rows + (1 - odd) + i
                place = X.at[h, dst, span(j), :]
                pltpu.make_async_remote_copy(
                    src_ref=place, dst_ref=place, send_sem=relay_send.at[h, j, i],
                    recv_sem=relay_recv.at[h, j, i],
                    device_id={"tile": relay_to}, device_id_type=MESH).wait_recv()

    def take(h, j):
        for i in range(rows):
            row_wait(h, j, i)
            if i < rows - 1:
                @pl.when(can_relay)
                def _():
                    relay_copy(h, j, i).start()

    for h in range(halves):
        load(h).wait()
        side_copy(h).start()
    for h in range(halves):
        side_copy(h).wait_recv()
        for j in range(pieces):
            for i in range(rows):
                row_copy(h, j, i).start()

    cond_copy(side, 2).wait_recv()

    @pl.when(has_above)
    def _():
        cond_copy(me - 2, 0).wait_recv()
        cond_copy(side - 2, 3).wait_recv()

    @pl.when(has_below)
    def _():
        cond_copy(me + 2, 1).wait_recv()
        cond_copy(side + 2, 4).wait_recv()

    first = lax.broadcasted_iota(jnp.int32, (2 * rows, LANES), 0) < rows

    def turned(above, here, below, j):
        lanes = slice(j * LANES, (j + 1) * LANES)
        top = jnp.where(first, C[above, :, lanes], C[here, :, lanes])
        blank = jnp.zeros((LANES - 4 * rows, LANES), jnp.float32)
        return jnp.transpose(jnp.concatenate([top, C[below, :, lanes], blank], 0))

    for j in range(cols // LANES):
        T[PAD + j * LANES:PAD + (j + 1) * LANES, :] = turned(0, 5, 1, j)
    for c in (0, TILE, width - PAD, width - TILE):
        T[c:c + TILE, :] = jnp.zeros((TILE, LANES), jnp.float32)

    @pl.when(core == 0)
    def _():
        T[width - PAD:width - TILE, :] = turned(3, 2, 4, 0)[0:TILE]

    @pl.when(core == 1)
    def _():
        T[TILE:PAD, :] = turned(3, 2, 4, cols // LANES - 1)[LANES - TILE:]

    def global_col(c):
        return core * cols - PAD + c + lax.broadcasted_iota(jnp.int32, (TILE, LANES), 0)

    global_row = chip * rows - rows + lax.broadcasted_iota(jnp.int32, (TILE, LANES), 1)
    total_rows, total_cols = chips * rows, 2 * cols

    def edges(t, _):
        c = pl.multiple_of(t * TILE, TILE)
        here = T[pl.ds(c, TILE), :]
        east = T[pl.ds(c + 1, TILE), :]
        south = pltpu.roll(here, LANES - 1, 1)
        gc = global_col(c)
        in_row = (global_row >= 0) & (global_row < total_rows - 1)
        TV[pl.ds(c, TILE), :] = jnp.where(in_row, 0.5 * (here + south), 0.0)
        in_col = (gc >= 0) & (gc < total_cols - 1)
        TH[pl.ds(c, TILE), :] = jnp.where(in_col, 0.5 * (here + east), 0.0)
        return 0

    TH[0:TILE, :] = jnp.zeros((TILE, LANES), jnp.float32)
    H[:, 0:TILE, :] = jnp.zeros((H.shape[0], TILE, LANES), jnp.float32)
    lax.fori_loop(1, width // TILE - 1, edges, 0)

    def spread(t, _):
        c = pl.multiple_of(t * TILE, TILE)
        at = pl.ds(c, TILE)
        v = TV[at, :]
        east = TH[at, :]
        west = TH[pl.ds(c - 1, TILE), :]
        diag = v + pltpu.roll(v, 1, 1) + east + west
        shape = (TILE, LANES)
        for k in range(2 * rows + 1):
            V[k, at, :] = jnp.broadcast_to(v[:, k + 1:k + 2], shape)
        for k in range(2 * rows):
            H[k, at, :] = jnp.broadcast_to(east[:, k + 2:k + 3], shape)
            D[k, at, :] = jnp.broadcast_to(diag[:, k + 2:k + 3], shape)
        return 0

    lax.fori_loop(1, width // TILE - 1, spread, 0)

    tiles = width // TILE

    def ends(lag, first, end):
        return [first] + [PAD // TILE - core + bound - lag for bound in bounds[1:-1]] + [end]

    r_ends = ends(1, 1, tiles - 1)
    w_ends = ends(2, 1, tiles - 1)
    u_ends = ends(3, 2, tiles - 2)

    def shape_of(cells, h, top):
        base = (chip * rows + top) * total_cols + core * cols - PAD
        return jnp.broadcast_to(cells[h:h + 1, :] - base, (TILE, LANES))

    def applied(ref, h, skip, count, c, low, grounds):
        at = pl.ds(c, TILE)
        west = pl.ds(c - 1, TILE)
        east = pl.ds(c + 1, TILE)
        column = c + lax.broadcasted_iota(jnp.int32, (TILE, LANES), 0)
        mid = ref[h, skip + 1, at, :]
        flow = V[low, at, :] * ref[h, skip, at, :]
        for k in range(count):
            after = ref[h, skip + k + 2, at, :]
            v = V[low + k + 1, at, :]
            grounded = column == grounds[k]
            diag = D[low + k, at, :]
            out = jnp.where(grounded, diag + 1.0, diag) * mid - flow
            out = out - v * after
            out = out - H[low + k, west, :] * ref[h, skip + 1 + k, west, :]
            out = out - H[low + k, at, :] * ref[h, skip + 1 + k, east, :]
            yield k, out, mid, grounded, column
            flow = v * mid
            mid = after

    def zeros():
        return tuple(jnp.zeros((TILE, LANES), jnp.float32) for _ in range(7))

    def compute(h, j, acc):
        def named(cells, top, count):
            return [shape_of(cells, h, top + k) for k in range(count)]

        count_r, count_w = 2 * rows, 2 * rows - 2
        src_r, gnd_r = named(source_ref, -2, count_r), named(ground_ref, -2, count_r)
        gnd_w = named(ground_ref, -1, count_w)
        src_u, gnd_u = named(source_ref, 0, rows), named(ground_ref, 0, rows)

        def pass_r(t, _):
            c = pl.multiple_of(t * TILE, TILE)
            for k, a, _mid, _g, column in applied(X, h, 1, count_r, c, 0, gnd_r):
                R[h, k, pl.ds(c, TILE), :] = jnp.where(column == src_r[k], 1.0 - a, -a)
            return 0

        def pass_w(t, _):
            c = pl.multiple_of(t * TILE, TILE)
            for k, a, _mid, _g, _column in applied(R, h, 0, count_w, c, 1, gnd_w):
                W[h, k, pl.ds(c, TILE), :] = a
            return 0

        def pass_u(t, acc):
            c = pl.multiple_of(t * TILE, TILE)
            at = pl.ds(c, TILE)
            for k, u, w, grounded, column in applied(W, h, 0, rows, c, 2, gnd_u):
                U[h, k, pl.ds(c - PAD, TILE), :] = u
                r = R[h, 2 + k, at, :]
                x = X[h, rows + k, at, :]
                sign = jnp.where(column == src_u[k], 1.0, 0.0) - jnp.where(grounded, 1.0, 0.0)
                terms = (r * r, r * w, w * w, w * u, sign * x, sign * r, sign * w)
                acc = tuple(s + term for s, term in zip(acc, terms))
            return acc

        lax.fori_loop(r_ends[j], r_ends[j + 1], pass_r, 0)
        lax.fori_loop(w_ends[j], w_ends[j + 1], pass_w, 0)
        return lax.fori_loop(u_ends[j], u_ends[j + 1], pass_u, acc)

    def keep(h, acc):
        sums = [jnp.sum(s, axis=0, keepdims=True) for s in acc]
        S[h, me] = jnp.concatenate(sums + [jnp.zeros((1, LANES), jnp.float32)], 0)

    def sum_copy(h, d):
        return pltpu.make_async_remote_copy(
            src_ref=S.at[h, me], dst_ref=S.at[h, me], send_sem=sum_send.at[h, d],
            recv_sem=sum_recv.at[h, d],
            device_id={"tile": (me + d) % n}, device_id_type=MESH)

    def send_sums(h):
        lax.fori_loop(1, n, lambda d, _: (sum_copy(h, d).start(), 0)[1], 0)

    def finish(h):
        def arrive(d, _):
            place = S.at[h, (me + n - d) % n]
            pltpu.make_async_remote_copy(
                src_ref=place, dst_ref=place, send_sem=sum_send.at[h, d],
                recv_sem=sum_recv.at[h, d], device_id={"tile": (me + d) % n},
                device_id_type=MESH).wait_recv()
            return 0

        lax.fori_loop(1, n, arrive, 0)
        total = S[h, 0]
        for k in range(1, n):
            total = total + S[h, k]
        m0, m1, m2, m3, ex, er, ew = (total[k:k + 1] for k in range(7))
        a0 = m0 / m1
        next_norm = a0 * (a0 * m2 - m1)
        ratio = next_norm / m0
        curve = m1 - a0 * (2.0 * m2 - a0 * m3)
        a1 = next_norm / (curve - ratio * next_norm / a0)
        p = a0 + a1 * (1.0 + ratio)
        q = a1 * a0
        drop_ref[h:h + 1, :] = ex + p * er - q * ew
        p3, q3 = p[None], q[None]

        lanes = slice(h * LANES, (h + 1) * LANES)
        p1 = jnp.broadcast_to(p, (TILE, LANES))
        q1 = jnp.broadcast_to(q, (TILE, LANES))

        def last(t, _):
            c = pl.multiple_of(t * TILE, TILE)
            at = pl.ds(c + PAD, TILE)
            to = pl.ds(c, TILE)
            for k in range(rows):
                r = R[h, 2 + k, at, :]
                w = W[h, 1 + k, at, :]
                pot_ref[0, k, to, lanes] = X[h, rows + k, at, :] + p1 * r - q1 * w
                res_ref[0, k, to, lanes] = r - p1 * w + q1 * U[h, k, to, :]
            return 0

        lax.fori_loop(0, cols // TILE, last, 0)

    order = [(h, j) for h in range(halves) for j in range(pieces)]
    acc = zeros()
    take(*order[0])
    for now, following in zip(order, order[1:] + [None]):
        h, j = now
        if following is not None:
            take(*following)
        relay_wait(h, j)
        acc = compute(h, j, acc)
        if j == pieces - 1:
            keep(h, acc)
            send_sums(h)
            acc = zeros()
        if h > 0 and j == 1:
            finish(h - 1)
    finish(halves - 1)

    cond_each(lambda copy: copy.wait_send())
    for h in range(halves):
        side_copy(h).wait_send()
        for j in range(pieces):
            for i in range(rows):
                row_copy(h, j, i).wait_send()

        @pl.when(can_relay)
        def _():
            for j in range(pieces):
                for i in range(rows - 1):
                    relay_copy(h, j, i).wait_send()

        lax.fori_loop(1, n, lambda d, _: (sum_copy(h, d).wait_send(), 0)[1], 0)


def solution(mesh):
    n = mesh.shape["tile"]

    def shards(habitat, table, source_cell, ground_cell, start_potential):
        _, rows, cols, rhs = start_potential.shape
        halves = rhs // LANES
        width = cols + 2 * PAD
        f32 = jnp.float32
        dma = pltpu.SemaphoreType.DMA
        field = jax.ShapeDtypeStruct(start_potential.shape, f32)
        vmem = pl.BlockSpec(memory_space=pltpu.VMEM)
        hbm = pl.BlockSpec(memory_space=pltpu.HBM)
        potentials, residual, drop = pl.pallas_call(
            functools.partial(kernel, n, rows, cols),
            out_shape=(field, field, jax.ShapeDtypeStruct((halves, LANES), f32)),
            in_specs=[pl.BlockSpec(memory_space=pltpu.SMEM), vmem, vmem, vmem, hbm],
            out_specs=(vmem, vmem, vmem),
            scratch_shapes=[
                pltpu.VMEM((halves, 3 * rows, width, LANES), f32),
                pltpu.VMEM((halves, 2 * rows, width, LANES), f32),
                pltpu.VMEM((halves, 2 * rows - 2, width, LANES), f32),
                pltpu.VMEM((halves, rows, cols, LANES), f32),
                pltpu.VMEM((2 * rows + 1, width, LANES), f32),
                pltpu.VMEM((2 * rows, width, LANES), f32),
                pltpu.VMEM((2 * rows, width, LANES), f32),
                pltpu.VMEM((6, 2 * rows, cols), f32),
                pltpu.VMEM((width, LANES), f32),
                pltpu.VMEM((width, LANES), f32),
                pltpu.VMEM((width, LANES), f32),
                pltpu.VMEM((halves, n, TILE, LANES), f32),
                dma((halves,)),
                dma((5,)), dma((5,)),
                dma((halves,)), dma((halves,)),
                dma((halves, 4, rows)), dma((halves, 4, rows)),
                dma((halves, 4, rows - 1)), dma((halves, 4, rows - 1)),
                dma((halves, n)), dma((halves, n)),
            ],
            compiler_params=pltpu.CompilerParams(
                collective_id=0, has_side_effects=True, vmem_limit_bytes=48 * 2**20),
        )(table, habitat, source_cell.reshape(halves, LANES),
          ground_cell.reshape(halves, LANES), start_potential)
        return potentials, residual, drop.reshape(rhs)

    placed = (
        P(("grp", "tile"), None, None),
        P(),
        P("grp"),
        P("grp"),
        P(("grp", "tile"), None, None, None),
    )
    return jax.shard_map(
        shards,
        mesh=mesh,
        in_specs=placed,
        out_specs=(placed[4], placed[4], P("grp")),
        check_vma=False,
    )
```

```python
import functools

import jax
import jax.numpy as jnp
from jax import lax
from jax.experimental import pallas as pl
from jax.experimental.pallas import tpu as pltpu
from jax.sharding import PartitionSpec as P

LANES = 128
TILE = 8
PAD = 2 * TILE
MESH = pl.DeviceIdType.MESH


def kernel(n, rows, cols, table_hbm, habitat_hbm, source_hbm, ground_hbm, start_ref,
           pot_ref, res_ref, drop_ref,
           X, R, W, U, V, H, D, C, T, TV, TH, S,
           table_ref, habitat_ref, source_ref, ground_ref, small_sem, load_sem, cond_send, cond_recv, side_send, side_recv,
           row_send, row_recv, relay_send, relay_recv, sum_send, sum_recv):
    halves = X.shape[0]
    width = cols + 2 * PAD
    me = lax.axis_index("tile")
    chips = n // 2
    chip = me // 2
    core = me % 2
    odd = chip % 2
    side = me + 1 - 2 * core
    partner = me + 2 - 4 * odd
    own = pl.ds(PAD, cols)
    travel = cols // TILE + 1
    bounds = [0, travel * 19 // 65, travel * 37 // 65, travel * 53 // 65, travel]
    pieces = len(bounds) - 1

    def load(h):
        return pltpu.make_async_copy(
            start_ref.at[0, :, :, pl.ds(h * LANES, LANES)], X.at[h, pl.ds(rows, rows), own, :],
            load_sem.at[h])

    smalls = [
        pltpu.make_async_copy(src, dst, small_sem.at[k])
        for k, (src, dst) in enumerate((
            (table_hbm, table_ref), (habitat_hbm, habitat_ref),
            (source_hbm, source_ref), (ground_hbm, ground_ref)))
    ]
    for copy in smalls:
        copy.start()
    for h in range(halves):
        load(h).start()

    barrier = pltpu.get_barrier_semaphore()

    def greet(d, _):
        pl.semaphore_signal(barrier, inc=1, device_id={"tile": (me + d) % n}, device_id_type=MESH)
        return 0

    for slot in range(5):
        C[slot] = jnp.zeros(C.shape[1:], jnp.float32)

    def zero(ref, lead, c):
        count = ref.shape[1]
        ref[lead[0], :, c:c + TILE, :] = jnp.zeros((count, TILE, LANES), jnp.float32)

    for h in range(halves):
        for c in (0, width - TILE):
            zero(X, (h,), c)
            zero(R, (h,), c)
            zero(W, (h,), c)
        @pl.when(core == 0)
        def _():
            zero(X, (h,), TILE)
        @pl.when(core == 1)
        def _():
            zero(X, (h,), width - PAD)
        @pl.when(chip == 0)
        def _():
            X[h, 0:rows] = jnp.zeros((rows, width, LANES), jnp.float32)
        @pl.when(chip == chips - 1)
        def _():
            X[h, 2 * rows:3 * rows] = jnp.zeros((rows, width, LANES), jnp.float32)

    lax.fori_loop(1, n, greet, 0)

    for copy in smalls:
        copy.wait()
    cells = habitat_ref[0]
    cond = jnp.zeros(cells.shape, jnp.float32)
    for level in range(table_ref.shape[0]):
        cond = jnp.where(cells == level, table_ref[level], cond)
    C[5, 0:rows, :] = cond
    C[5, rows:2 * rows, :] = cond

    pl.semaphore_wait(barrier, n - 1)

    def cond_copy(target, slot):
        return pltpu.make_async_remote_copy(
            src_ref=C.at[5], dst_ref=C.at[slot], send_sem=cond_send.at[slot],
            recv_sem=cond_recv.at[slot], device_id={"tile": target}, device_id_type=MESH)

    has_above = chip > 0
    has_below = chip < chips - 1

    def cond_each(act):
        act(cond_copy(side, 2))

        @pl.when(has_above)
        def _():
            act(cond_copy(me - 2, 1))
            act(cond_copy(side - 2, 4))

        @pl.when(has_below)
        def _():
            act(cond_copy(me + 2, 0))
            act(cond_copy(side + 2, 3))

    cond_each(lambda copy: copy.start())

    inner = pl.multiple_of(PAD + (1 - core) * (cols - TILE), TILE)

    def side_copy(h):
        dst = pl.multiple_of((1 - core) * TILE + core * (PAD + cols), TILE)
        return pltpu.make_async_remote_copy(
            src_ref=X.at[h, pl.ds(rows, rows), pl.ds(inner, TILE), :],
            dst_ref=X.at[h, pl.ds(rows, rows), pl.ds(dst, TILE), :],
            send_sem=side_send.at[h], recv_sem=side_recv.at[h],
            device_id={"tile": side}, device_id_type=MESH)

    def span(j):
        start = pl.multiple_of(PAD - core * TILE + bounds[j] * TILE, TILE)
        return pl.ds(start, (bounds[j + 1] - bounds[j]) * TILE)

    def row_copy(h, j, i):
        r = (i + odd) % rows
        return pltpu.make_async_remote_copy(
            src_ref=X.at[h, rows + r, span(j), :],
            dst_ref=X.at[h, odd * 2 * rows + r, span(j), :],
            send_sem=row_send.at[h, j, i], recv_sem=row_recv.at[h, j, i],
            device_id={"tile": partner}, device_id_type=MESH)

    def row_wait(h, j, i):
        r = (i + 1 - odd) % rows
        place = X.at[h, (1 - odd) * 2 * rows + r, span(j), :]
        pltpu.make_async_remote_copy(
            src_ref=place, dst_ref=place,
            send_sem=row_send.at[h, j, i], recv_sem=row_recv.at[h, j, i],
            device_id={"tile": partner}, device_id_type=MESH).wait_recv()

    relay_to = me + 4 - 8 * odd
    can_relay = jnp.where(odd == 0, chip + 2 < chips, chip >= 2)
    gets_relay = jnp.where(odd == 0, chip >= 2, chip + 2 < chips)

    def relay_copy(h, j, i):
        src = (1 - odd) * (2 * rows + 1) + i
        dst = odd * 2 * rows + (1 - odd) + i
        return pltpu.make_async_remote_copy(
            src_ref=X.at[h, src, span(j), :], dst_ref=X.at[h, dst, span(j), :],
            send_sem=relay_send.at[h, j, i], recv_sem=relay_recv.at[h, j, i],
            device_id={"tile": relay_to}, device_id_type=MESH)

    def relay_wait(h, j):
        @pl.when(gets_relay)
        def _():
            for i in range(rows - 1):
                dst = odd * 2 * rows + (1 - odd) + i
                place = X.at[h, dst, span(j), :]
                pltpu.make_async_remote_copy(
                    src_ref=place, dst_ref=place, send_sem=relay_send.at[h, j, i],
                    recv_sem=relay_recv.at[h, j, i],
                    device_id={"tile": relay_to}, device_id_type=MESH).wait_recv()

    order = [(h, j) for h in range(halves) for j in range(pieces)]
    arrivals = [(h, j, i) for h, j in order for i in range(rows)]

    def take(count):
        for h, j, i in arrivals[:count]:
            row_wait(h, j, i)
            if i < rows - 1:
                @pl.when(can_relay)
                def _():
                    relay_copy(h, j, i).start()
        del arrivals[:count]

    for h in range(halves):
        load(h).wait()
        side_copy(h).start()
        for j in range(pieces):
            if j in (0, pieces - 1):
                @pl.when(core == (1 if j == 0 else 0))
                def _():
                    side_copy(h).wait_recv()
            for i in range(rows):
                row_copy(h, j, i).start()

    cond_copy(side, 2).wait_recv()

    @pl.when(has_above)
    def _():
        cond_copy(me - 2, 0).wait_recv()
        cond_copy(side - 2, 3).wait_recv()

    @pl.when(has_below)
    def _():
        cond_copy(me + 2, 1).wait_recv()
        cond_copy(side + 2, 4).wait_recv()

    first = lax.broadcasted_iota(jnp.int32, (2 * rows, LANES), 0) < rows

    def turned(above, here, below, j):
        lanes = slice(j * LANES, (j + 1) * LANES)
        top = jnp.where(first, C[above, :, lanes], C[here, :, lanes])
        blank = jnp.zeros((LANES - 4 * rows, LANES), jnp.float32)
        return jnp.transpose(jnp.concatenate([top, C[below, :, lanes], blank], 0))

    for j in range(cols // LANES):
        T[PAD + j * LANES:PAD + (j + 1) * LANES, :] = turned(0, 5, 1, j)
    for c in (0, TILE, width - PAD, width - TILE):
        T[c:c + TILE, :] = jnp.zeros((TILE, LANES), jnp.float32)

    @pl.when(core == 0)
    def _():
        T[width - PAD:width - TILE, :] = turned(3, 2, 4, 0)[0:TILE]

    @pl.when(core == 1)
    def _():
        T[TILE:PAD, :] = turned(3, 2, 4, cols // LANES - 1)[LANES - TILE:]

    def global_col(c):
        return core * cols - PAD + c + lax.broadcasted_iota(jnp.int32, (TILE, LANES), 0)

    global_row = chip * rows - rows + lax.broadcasted_iota(jnp.int32, (TILE, LANES), 1)
    total_rows, total_cols = chips * rows, 2 * cols

    def edges(t, _):
        c = pl.multiple_of(t * TILE, TILE)
        here = T[pl.ds(c, TILE), :]
        east = T[pl.ds(c + 1, TILE), :]
        south = pltpu.roll(here, LANES - 1, 1)
        gc = global_col(c)
        in_row = (global_row >= 0) & (global_row < total_rows - 1)
        TV[pl.ds(c, TILE), :] = jnp.where(in_row, 0.5 * (here + south), 0.0)
        in_col = (gc >= 0) & (gc < total_cols - 1)
        TH[pl.ds(c, TILE), :] = jnp.where(in_col, 0.5 * (here + east), 0.0)
        return 0

    TH[0:TILE, :] = jnp.zeros((TILE, LANES), jnp.float32)
    H[:, 0:TILE, :] = jnp.zeros((H.shape[0], TILE, LANES), jnp.float32)
    lax.fori_loop(1, width // TILE - 1, edges, 0, unroll=2)
    take(2)

    def spread(t, _):
        c = pl.multiple_of(t * TILE, TILE)
        at = pl.ds(c, TILE)
        v = TV[at, :]
        east = TH[at, :]
        west = TH[pl.ds(c - 1, TILE), :]
        diag = v + pltpu.roll(v, 1, 1) + east + west
        shape = (TILE, LANES)
        for k in range(2 * rows + 1):
            V[k, at, :] = jnp.broadcast_to(v[:, k + 1:k + 2], shape)
        for k in range(2 * rows):
            H[k, at, :] = jnp.broadcast_to(east[:, k + 2:k + 3], shape)
            D[k, at, :] = jnp.broadcast_to(diag[:, k + 2:k + 3], shape)
        return 0

    parts = 6
    for part in range(parts):
        step = (width // TILE - 2) // parts
        stop = width // TILE - 1 if part == parts - 1 else 1 + (part + 1) * step
        lax.fori_loop(1 + part * step, stop, spread, 0)
        take(1)

    tiles = width // TILE

    def ends(lag, first, end):
        return [first] + [PAD // TILE - core + bound - lag for bound in bounds[1:-1]] + [end]

    r_ends = ends(1, 1, tiles - 1)
    w_ends = ends(2, 1, tiles - 1)
    u_ends = ends(3, 2, tiles - 2)

    def shape_of(cells, h, top):
        base = (chip * rows + top) * total_cols + core * cols - PAD
        return jnp.broadcast_to(cells[h:h + 1, :] - base, (TILE, LANES))

    def applied(ref, h, skip, count, c, low, grounds):
        at = pl.ds(c, TILE)
        west = pl.ds(c - 1, TILE)
        east = pl.ds(c + 1, TILE)
        column = c + lax.broadcasted_iota(jnp.int32, (TILE, LANES), 0)
        mid = ref[h, skip + 1, at, :]
        flow = V[low, at, :] * ref[h, skip, at, :]
        for k in range(count):
            after = ref[h, skip + k + 2, at, :]
            v = V[low + k + 1, at, :]
            grounded = column == grounds[k]
            diag = D[low + k, at, :]
            out = jnp.where(grounded, diag + 1.0, diag) * mid - flow
            out = out - v * after
            out = out - H[low + k, west, :] * ref[h, skip + 1 + k, west, :]
            out = out - H[low + k, at, :] * ref[h, skip + 1 + k, east, :]
            yield k, out, mid, grounded, column
            flow = v * mid
            mid = after

    def zeros():
        return tuple(jnp.zeros((TILE, LANES), jnp.float32) for _ in range(7))

    def compute(h, j, acc):
        def named(cells, top, count):
            return [shape_of(cells, h, top + k) for k in range(count)]

        count_r, count_w = 2 * rows, 2 * rows - 2
        src_r, gnd_r = named(source_ref, -2, count_r), named(ground_ref, -2, count_r)
        gnd_w = named(ground_ref, -1, count_w)
        src_u, gnd_u = named(source_ref, 0, rows), named(ground_ref, 0, rows)

        def pass_r(t, _):
            c = pl.multiple_of(t * TILE, TILE)
            for k, a, _mid, _g, column in applied(X, h, 1, count_r, c, 0, gnd_r):
                R[h, k, pl.ds(c, TILE), :] = jnp.where(column == src_r[k], 1.0 - a, -a)
            return 0

        def pass_w(t, _):
            c = pl.multiple_of(t * TILE, TILE)
            for k, a, _mid, _g, _column in applied(R, h, 0, count_w, c, 1, gnd_w):
                W[h, k, pl.ds(c, TILE), :] = a
            return 0

        def pass_u(t, acc):
            c = pl.multiple_of(t * TILE, TILE)
            at = pl.ds(c, TILE)
            for k, u, w, grounded, column in applied(W, h, 0, rows, c, 2, gnd_u):
                U[h, k, pl.ds(c - PAD, TILE), :] = u
                r = R[h, 2 + k, at, :]
                x = X[h, rows + k, at, :]
                sign = jnp.where(column == src_u[k], 1.0, 0.0) - jnp.where(grounded, 1.0, 0.0)
                terms = (r * r, r * w, w * w, w * u, sign * x, sign * r, sign * w)
                acc = tuple(s + term for s, term in zip(acc, terms))
            return acc

        lax.fori_loop(r_ends[j], r_ends[j + 1], pass_r, 0)
        lax.fori_loop(w_ends[j], w_ends[j + 1], pass_w, 0)
        return lax.fori_loop(u_ends[j], u_ends[j + 1], pass_u, acc)

    def keep(h, acc):
        sums = [jnp.sum(s, axis=0, keepdims=True) for s in acc]
        S[h, me] = jnp.concatenate(sums + [jnp.zeros((1, LANES), jnp.float32)], 0)

    def sum_copy(h, d):
        return pltpu.make_async_remote_copy(
            src_ref=S.at[h, me], dst_ref=S.at[h, me], send_sem=sum_send.at[h, d],
            recv_sem=sum_recv.at[h, d],
            device_id={"tile": (me + d) % n}, device_id_type=MESH)

    def send_sums(h):
        lax.fori_loop(1, n, lambda d, _: (sum_copy(h, d).start(), 0)[1], 0)

    def finish(h):
        def arrive(d, _):
            place = S.at[h, (me + n - d) % n]
            pltpu.make_async_remote_copy(
                src_ref=place, dst_ref=place, send_sem=sum_send.at[h, d],
                recv_sem=sum_recv.at[h, d], device_id={"tile": (me + d) % n},
                device_id_type=MESH).wait_recv()
            return 0

        lax.fori_loop(1, n, arrive, 0)
        total = S[h, 0]
        for k in range(1, n):
            total = total + S[h, k]
        m0, m1, m2, m3, ex, er, ew = (total[k:k + 1] for k in range(7))
        a0 = m0 / m1
        next_norm = a0 * (a0 * m2 - m1)
        ratio = next_norm / m0
        curve = m1 - a0 * (2.0 * m2 - a0 * m3)
        a1 = next_norm / (curve - ratio * next_norm / a0)
        p = a0 + a1 * (1.0 + ratio)
        q = a1 * a0
        drop_ref[h:h + 1, :] = ex + p * er - q * ew
        p3, q3 = p[None], q[None]

        lanes = slice(h * LANES, (h + 1) * LANES)
        p1 = jnp.broadcast_to(p, (TILE, LANES))
        q1 = jnp.broadcast_to(q, (TILE, LANES))

        def last(t, _):
            c = pl.multiple_of(t * TILE, TILE)
            at = pl.ds(c + PAD, TILE)
            to = pl.ds(c, TILE)
            for k in range(rows):
                r = R[h, 2 + k, at, :]
                w = W[h, 1 + k, at, :]
                pot_ref[0, k, to, lanes] = X[h, rows + k, at, :] + p1 * r - q1 * w
                res_ref[0, k, to, lanes] = r - p1 * w + q1 * U[h, k, to, :]
            return 0

        lax.fori_loop(0, cols // TILE, last, 0)

    acc = zeros()
    for k, (h, j) in enumerate(order):
        take(max(0, len(arrivals) - rows * max(0, len(order) - k - 2)))
        relay_wait(h, j)
        acc = compute(h, j, acc)
        if j == pieces - 1:
            keep(h, acc)
            send_sums(h)
            acc = zeros()
        if h > 0 and j == 1:
            finish(h - 1)
    finish(halves - 1)

    cond_each(lambda copy: copy.wait_send())
    for h in range(halves):
        side_copy(h).wait_send()
        for j in range(pieces):
            for i in range(rows):
                row_copy(h, j, i).wait_send()

        @pl.when(can_relay)
        def _():
            for j in range(pieces):
                for i in range(rows - 1):
                    relay_copy(h, j, i).wait_send()

        lax.fori_loop(1, n, lambda d, _: (sum_copy(h, d).wait_send(), 0)[1], 0)


def solution(mesh):
    n = mesh.shape["tile"]

    def shards(habitat, table, source_cell, ground_cell, start_potential):
        _, rows, cols, rhs = start_potential.shape
        halves = rhs // LANES
        width = cols + 2 * PAD
        f32 = jnp.float32
        dma = pltpu.SemaphoreType.DMA
        field = jax.ShapeDtypeStruct(start_potential.shape, f32)
        vmem = pl.BlockSpec(memory_space=pltpu.VMEM)
        hbm = pl.BlockSpec(memory_space=pltpu.HBM)
        potentials, residual, drop = pl.pallas_call(
            functools.partial(kernel, n, rows, cols),
            out_shape=(field, field, jax.ShapeDtypeStruct((halves, LANES), f32)),
            in_specs=[hbm] * 5,
            out_specs=(vmem, vmem, vmem),
            scratch_shapes=[
                pltpu.VMEM((halves, 3 * rows, width, LANES), f32),
                pltpu.VMEM((halves, 2 * rows, width, LANES), f32),
                pltpu.VMEM((halves, 2 * rows - 2, width, LANES), f32),
                pltpu.VMEM((halves, rows, cols, LANES), f32),
                pltpu.VMEM((2 * rows + 1, width, LANES), f32),
                pltpu.VMEM((2 * rows, width, LANES), f32),
                pltpu.VMEM((2 * rows, width, LANES), f32),
                pltpu.VMEM((6, 2 * rows, cols), f32),
                pltpu.VMEM((width, LANES), f32),
                pltpu.VMEM((width, LANES), f32),
                pltpu.VMEM((width, LANES), f32),
                pltpu.VMEM((halves, n, TILE, LANES), f32),
                pltpu.SMEM(table.shape, f32),
                pltpu.VMEM(habitat.shape, jnp.int32),
                pltpu.VMEM((halves, LANES), jnp.int32),
                pltpu.VMEM((halves, LANES), jnp.int32),
                dma((4,)),
                dma((halves,)),
                dma((5,)), dma((5,)),
                dma((halves,)), dma((halves,)),
                dma((halves, 4, rows)), dma((halves, 4, rows)),
                dma((halves, 4, rows - 1)), dma((halves, 4, rows - 1)),
                dma((halves, n)), dma((halves, n)),
            ],
            compiler_params=pltpu.CompilerParams(
                collective_id=0, has_side_effects=True, vmem_limit_bytes=48 * 2**20),
        )(*(pltpu.with_memory_space_constraint(value, pltpu.HBM) for value in (
            table, habitat, source_cell.reshape(halves, LANES),
            ground_cell.reshape(halves, LANES), start_potential)))
        return potentials, residual, drop.reshape(rhs)

    placed = (
        P(("grp", "tile"), None, None),
        P(),
        P("grp"),
        P("grp"),
        P(("grp", "tile"), None, None, None),
    )
    return jax.shard_map(
        shards,
        mesh=mesh,
        in_specs=placed,
        out_specs=(placed[4], placed[4], P("grp")),
        check_vma=False,
    )
```

```python
import functools

import jax
import jax.numpy as jnp
from jax import lax
from jax.experimental import pallas as pl
from jax.experimental.pallas import tpu as pltpu
from jax.sharding import PartitionSpec as P

LANES = 128
TILE = 8
PAD = 2 * TILE
MESH = pl.DeviceIdType.MESH


def kernel(n, rows, cols, table_hbm, habitat_hbm, source_hbm, ground_hbm, start_ref,
           pot_ref, res_ref, drop_ref,
           X, R, W, U, V, H, D, C, T, TV, TH, S,
           table_ref, habitat_ref, source_ref, ground_ref, small_sem, load_sem, cond_send, cond_recv, side_send, side_recv,
           row_send, row_recv, relay_send, relay_recv, sum_send, sum_recv):
    halves = X.shape[0]
    width = cols + 2 * PAD
    me = lax.axis_index("tile")
    chips = n // 2
    chip = me // 2
    core = me % 2
    odd = chip % 2
    side = me + 1 - 2 * core
    partner = me + 2 - 4 * odd
    own = pl.ds(PAD, cols)
    travel = cols // TILE + 1
    bounds = [0, travel * 19 // 65, travel * 37 // 65, travel * 53 // 65, travel]
    pieces = len(bounds) - 1

    def load(h):
        return pltpu.make_async_copy(
            start_ref.at[0, :, :, pl.ds(h * LANES, LANES)], X.at[h, pl.ds(rows, rows), own, :],
            load_sem.at[h])

    smalls = [
        pltpu.make_async_copy(src, dst, small_sem.at[k])
        for k, (src, dst) in enumerate((
            (table_hbm, table_ref), (habitat_hbm, habitat_ref),
            (source_hbm, source_ref), (ground_hbm, ground_ref)))
    ]
    for copy in smalls:
        copy.start()
    for h in range(halves):
        load(h).start()

    barrier = pltpu.get_barrier_semaphore()

    def greet(d, _):
        pl.semaphore_signal(barrier, inc=1, device_id={"tile": (me + d) % n}, device_id_type=MESH)
        return 0

    for slot in range(5):
        C[slot] = jnp.zeros(C.shape[1:], jnp.float32)

    def zero(ref, lead, c):
        count = ref.shape[1]
        ref[lead[0], :, c:c + TILE, :] = jnp.zeros((count, TILE, LANES), jnp.float32)

    lax.fori_loop(1, n, greet, 0)

    for copy in smalls:
        copy.wait()
    cells = habitat_ref[0]
    cond = jnp.zeros(cells.shape, jnp.float32)
    for level in range(table_ref.shape[0]):
        cond = jnp.where(cells == level, table_ref[level], cond)
    C[5, 0:rows, :] = cond
    C[5, rows:2 * rows, :] = cond

    pl.semaphore_wait(barrier, n - 1)

    def cond_copy(target, slot):
        return pltpu.make_async_remote_copy(
            src_ref=C.at[5], dst_ref=C.at[slot], send_sem=cond_send.at[slot],
            recv_sem=cond_recv.at[slot], device_id={"tile": target}, device_id_type=MESH)

    has_above = chip > 0
    has_below = chip < chips - 1

    def cond_each(act):
        act(cond_copy(side, 2))

        @pl.when(has_above)
        def _():
            act(cond_copy(me - 2, 1))
            act(cond_copy(side - 2, 4))

        @pl.when(has_below)
        def _():
            act(cond_copy(me + 2, 0))
            act(cond_copy(side + 2, 3))

    cond_each(lambda copy: copy.start())

    inner = pl.multiple_of(PAD + (1 - core) * (cols - TILE), TILE)

    def side_copy(h):
        dst = pl.multiple_of((1 - core) * TILE + core * (PAD + cols), TILE)
        return pltpu.make_async_remote_copy(
            src_ref=X.at[h, pl.ds(rows, rows), pl.ds(inner, TILE), :],
            dst_ref=X.at[h, pl.ds(rows, rows), pl.ds(dst, TILE), :],
            send_sem=side_send.at[h], recv_sem=side_recv.at[h],
            device_id={"tile": side}, device_id_type=MESH)

    def span(j):
        start = pl.multiple_of(PAD - core * TILE + bounds[j] * TILE, TILE)
        return pl.ds(start, (bounds[j + 1] - bounds[j]) * TILE)

    def row_copy(h, j, i):
        r = (i + odd) % rows
        return pltpu.make_async_remote_copy(
            src_ref=X.at[h, rows + r, span(j), :],
            dst_ref=X.at[h, odd * 2 * rows + r, span(j), :],
            send_sem=row_send.at[h, j, i], recv_sem=row_recv.at[h, j, i],
            device_id={"tile": partner}, device_id_type=MESH)

    def row_wait(h, j, i):
        r = (i + 1 - odd) % rows
        place = X.at[h, (1 - odd) * 2 * rows + r, span(j), :]
        pltpu.make_async_remote_copy(
            src_ref=place, dst_ref=place,
            send_sem=row_send.at[h, j, i], recv_sem=row_recv.at[h, j, i],
            device_id={"tile": partner}, device_id_type=MESH).wait_recv()

    relay_to = me + 4 - 8 * odd
    can_relay = jnp.where(odd == 0, chip + 2 < chips, chip >= 2)
    gets_relay = jnp.where(odd == 0, chip >= 2, chip + 2 < chips)

    def relay_copy(h, j, i):
        src = (1 - odd) * (2 * rows + 1) + i
        dst = odd * 2 * rows + (1 - odd) + i
        return pltpu.make_async_remote_copy(
            src_ref=X.at[h, src, span(j), :], dst_ref=X.at[h, dst, span(j), :],
            send_sem=relay_send.at[h, j, i], recv_sem=relay_recv.at[h, j, i],
            device_id={"tile": relay_to}, device_id_type=MESH)

    def relay_wait(h, j):
        @pl.when(gets_relay)
        def _():
            for i in range(rows - 1):
                dst = odd * 2 * rows + (1 - odd) + i
                place = X.at[h, dst, span(j), :]
                pltpu.make_async_remote_copy(
                    src_ref=place, dst_ref=place, send_sem=relay_send.at[h, j, i],
                    recv_sem=relay_recv.at[h, j, i],
                    device_id={"tile": relay_to}, device_id_type=MESH).wait_recv()

    order = [(h, j) for h in range(halves) for j in range(pieces)]
    arrivals = [(h, j, i) for h, j in order[:-2] for i in range(rows)]
    arrivals += [(h, j, i) for h, j in order[-2:] for i in range(rows - 1)]
    arrivals += [(h, j, rows - 1) for h, j in order[-2:]]

    def take(count):
        for h, j, i in arrivals[:count]:
            row_wait(h, j, i)
            if i < rows - 1:
                @pl.when(can_relay)
                def _():
                    relay_copy(h, j, i).start()
        del arrivals[:count]

    for h in range(halves):
        load(h).wait()
        side_copy(h).start()
        for j, i in [place[1:] for place in arrivals if place[0] == h]:
            if i == 0 and j in (0, pieces - 1):
                @pl.when(core == (1 if j == 0 else 0))
                def _():
                    side_copy(h).wait_recv()
            row_copy(h, j, i).start()

    for h in range(halves):
        for c in (0, width - TILE):
            zero(X, (h,), c)
            zero(R, (h,), c)
            zero(W, (h,), c)
        @pl.when(core == 0)
        def _():
            zero(X, (h,), TILE)
        @pl.when(core == 1)
        def _():
            zero(X, (h,), width - PAD)
        @pl.when(chip == 0)
        def _():
            X[h, 0:rows] = jnp.zeros((rows, width, LANES), jnp.float32)
        @pl.when(chip == chips - 1)
        def _():
            X[h, 2 * rows:3 * rows] = jnp.zeros((rows, width, LANES), jnp.float32)

    cond_copy(side, 2).wait_recv()

    @pl.when(has_above)
    def _():
        cond_copy(me - 2, 0).wait_recv()
        cond_copy(side - 2, 3).wait_recv()

    @pl.when(has_below)
    def _():
        cond_copy(me + 2, 1).wait_recv()
        cond_copy(side + 2, 4).wait_recv()

    first = lax.broadcasted_iota(jnp.int32, (2 * rows, LANES), 0) < rows

    def turned(above, here, below, j):
        lanes = slice(j * LANES, (j + 1) * LANES)
        top = jnp.where(first, C[above, :, lanes], C[here, :, lanes])
        blank = jnp.zeros((LANES - 4 * rows, LANES), jnp.float32)
        return jnp.transpose(jnp.concatenate([top, C[below, :, lanes], blank], 0))

    for j in range(cols // LANES):
        T[PAD + j * LANES:PAD + (j + 1) * LANES, :] = turned(0, 5, 1, j)
    for c in (0, TILE, width - PAD, width - TILE):
        T[c:c + TILE, :] = jnp.zeros((TILE, LANES), jnp.float32)

    @pl.when(core == 0)
    def _():
        T[width - PAD:width - TILE, :] = turned(3, 2, 4, 0)[0:TILE]

    @pl.when(core == 1)
    def _():
        T[TILE:PAD, :] = turned(3, 2, 4, cols // LANES - 1)[LANES - TILE:]

    def global_col(c):
        return core * cols - PAD + c + lax.broadcasted_iota(jnp.int32, (TILE, LANES), 0)

    global_row = chip * rows - rows + lax.broadcasted_iota(jnp.int32, (TILE, LANES), 1)
    total_rows, total_cols = chips * rows, 2 * cols

    def edges(t, _):
        c = pl.multiple_of(t * TILE, TILE)
        here = T[pl.ds(c, TILE), :]
        east = T[pl.ds(c + 1, TILE), :]
        south = pltpu.roll(here, LANES - 1, 1)
        gc = global_col(c)
        in_row = (global_row >= 0) & (global_row < total_rows - 1)
        TV[pl.ds(c, TILE), :] = jnp.where(in_row, 0.5 * (here + south), 0.0)
        in_col = (gc >= 0) & (gc < total_cols - 1)
        TH[pl.ds(c, TILE), :] = jnp.where(in_col, 0.5 * (here + east), 0.0)
        return 0

    TH[0:TILE, :] = jnp.zeros((TILE, LANES), jnp.float32)
    H[:, 0:TILE, :] = jnp.zeros((H.shape[0], TILE, LANES), jnp.float32)
    lax.fori_loop(1, width // TILE - 1, edges, 0, unroll=2)
    take(2)

    def spread(t, _):
        c = pl.multiple_of(t * TILE, TILE)
        at = pl.ds(c, TILE)
        v = TV[at, :]
        east = TH[at, :]
        west = TH[pl.ds(c - 1, TILE), :]
        diag = v + pltpu.roll(v, 1, 1) + east + west
        shape = (TILE, LANES)
        for k in range(2 * rows + 1):
            V[k, at, :] = jnp.broadcast_to(v[:, k + 1:k + 2], shape)
        for k in range(2 * rows):
            H[k, at, :] = jnp.broadcast_to(east[:, k + 2:k + 3], shape)
            D[k, at, :] = jnp.broadcast_to(diag[:, k + 2:k + 3], shape)
        return 0

    parts = 6
    for part in range(parts):
        step = (width // TILE - 2) // parts
        stop = width // TILE - 1 if part == parts - 1 else 1 + (part + 1) * step
        lax.fori_loop(1 + part * step, stop, spread, 0)
        take(1)

    tiles = width // TILE

    def ends(lag, first, end):
        return [first] + [PAD // TILE - core + bound - lag for bound in bounds[1:-1]] + [end]

    r_ends = ends(1, 1, tiles - 1)
    w_ends = ends(2, 1, tiles - 1)
    u_ends = ends(3, 2, tiles - 2)

    def shape_of(cells, h, top):
        base = (chip * rows + top) * total_cols + core * cols - PAD
        return jnp.broadcast_to(cells[h:h + 1, :] - base, (TILE, LANES))

    def applied(ref, h, skip, count, c, low, grounds):
        at = pl.ds(c, TILE)
        west = pl.ds(c - 1, TILE)
        east = pl.ds(c + 1, TILE)
        column = c + lax.broadcasted_iota(jnp.int32, (TILE, LANES), 0)
        mid = ref[h, skip + 1, at, :]
        flow = V[low, at, :] * ref[h, skip, at, :]
        for k in range(count):
            after = ref[h, skip + k + 2, at, :]
            v = V[low + k + 1, at, :]
            grounded = column == grounds[k]
            diag = D[low + k, at, :]
            out = jnp.where(grounded, diag + 1.0, diag) * mid - flow
            out = out - v * after
            out = out - H[low + k, west, :] * ref[h, skip + 1 + k, west, :]
            out = out - H[low + k, at, :] * ref[h, skip + 1 + k, east, :]
            yield k, out, mid, grounded, column
            flow = v * mid
            mid = after

    def zeros():
        return tuple(jnp.zeros((TILE, LANES), jnp.float32) for _ in range(7))

    def compute(h, j, acc):
        def named(cells, top, count):
            return [shape_of(cells, h, top + k) for k in range(count)]

        count_r, count_w = 2 * rows, 2 * rows - 2
        src_r, gnd_r = named(source_ref, -2, count_r), named(ground_ref, -2, count_r)
        gnd_w = named(ground_ref, -1, count_w)
        src_u, gnd_u = named(source_ref, 0, rows), named(ground_ref, 0, rows)

        def pass_r(t, _):
            c = pl.multiple_of(t * TILE, TILE)
            for k, a, _mid, _g, column in applied(X, h, 1, count_r, c, 0, gnd_r):
                R[h, k, pl.ds(c, TILE), :] = jnp.where(column == src_r[k], 1.0 - a, -a)
            return 0

        def pass_w(t, _):
            c = pl.multiple_of(t * TILE, TILE)
            for k, a, _mid, _g, _column in applied(R, h, 0, count_w, c, 1, gnd_w):
                W[h, k, pl.ds(c, TILE), :] = a
            return 0

        def pass_u(t, acc):
            c = pl.multiple_of(t * TILE, TILE)
            at = pl.ds(c, TILE)
            for k, u, w, grounded, column in applied(W, h, 0, rows, c, 2, gnd_u):
                U[h, k, pl.ds(c - PAD, TILE), :] = u
                r = R[h, 2 + k, at, :]
                x = X[h, rows + k, at, :]
                sign = jnp.where(column == src_u[k], 1.0, 0.0) - jnp.where(grounded, 1.0, 0.0)
                terms = (r * r, r * w, w * w, w * u, sign * x, sign * r, sign * w)
                acc = tuple(s + term for s, term in zip(acc, terms))
            return acc

        lax.fori_loop(r_ends[j], r_ends[j + 1], pass_r, 0)
        lax.fori_loop(w_ends[j], w_ends[j + 1], pass_w, 0)
        return lax.fori_loop(u_ends[j], u_ends[j + 1], pass_u, acc)

    def keep(h, acc):
        sums = [jnp.sum(s, axis=0, keepdims=True) for s in acc]
        S[h, me] = jnp.concatenate(sums + [jnp.zeros((1, LANES), jnp.float32)], 0)

    def sum_copy(h, d):
        return pltpu.make_async_remote_copy(
            src_ref=S.at[h, me], dst_ref=S.at[h, me], send_sem=sum_send.at[h, d],
            recv_sem=sum_recv.at[h, d],
            device_id={"tile": (me + d) % n}, device_id_type=MESH)

    def send_sums(h):
        lax.fori_loop(1, n, lambda d, _: (sum_copy(h, d).start(), 0)[1], 0)

    def finish(h):
        def arrive(d, _):
            place = S.at[h, (me + n - d) % n]
            pltpu.make_async_remote_copy(
                src_ref=place, dst_ref=place, send_sem=sum_send.at[h, d],
                recv_sem=sum_recv.at[h, d], device_id={"tile": (me + d) % n},
                device_id_type=MESH).wait_recv()
            return 0

        lax.fori_loop(1, n, arrive, 0)
        total = S[h, 0]
        for k in range(1, n):
            total = total + S[h, k]
        m0, m1, m2, m3, ex, er, ew = (total[k:k + 1] for k in range(7))
        a0 = m0 / m1
        next_norm = a0 * (a0 * m2 - m1)
        ratio = next_norm / m0
        curve = m1 - a0 * (2.0 * m2 - a0 * m3)
        a1 = next_norm / (curve - ratio * next_norm / a0)
        p = a0 + a1 * (1.0 + ratio)
        q = a1 * a0
        drop_ref[h:h + 1, :] = ex + p * er - q * ew
        p3, q3 = p[None], q[None]

        lanes = slice(h * LANES, (h + 1) * LANES)
        p1 = jnp.broadcast_to(p, (TILE, LANES))
        q1 = jnp.broadcast_to(q, (TILE, LANES))

        def last(t, _):
            c = pl.multiple_of(t * TILE, TILE)
            at = pl.ds(c + PAD, TILE)
            to = pl.ds(c, TILE)
            for k in range(rows):
                r = R[h, 2 + k, at, :]
                w = W[h, 1 + k, at, :]
                pot_ref[0, k, to, lanes] = X[h, rows + k, at, :] + p1 * r - q1 * w
                res_ref[0, k, to, lanes] = r - p1 * w + q1 * U[h, k, to, :]
            return 0

        lax.fori_loop(0, cols // TILE, last, 0)

    acc = zeros()
    for k, (h, j) in enumerate(order):
        left = len(order) - k - 1
        take(len(arrivals) - (left if left < 2 else rows * (left - 1)))
        relay_wait(h, j)
        acc = compute(h, j, acc)
        if j == pieces - 1:
            keep(h, acc)
            send_sums(h)
            acc = zeros()
        if h > 0 and j == 1:
            finish(h - 1)
    finish(halves - 1)

    cond_each(lambda copy: copy.wait_send())
    for h in range(halves):
        side_copy(h).wait_send()
        for j in range(pieces):
            for i in range(rows):
                row_copy(h, j, i).wait_send()

        @pl.when(can_relay)
        def _():
            for j in range(pieces):
                for i in range(rows - 1):
                    relay_copy(h, j, i).wait_send()

        lax.fori_loop(1, n, lambda d, _: (sum_copy(h, d).wait_send(), 0)[1], 0)


def solution(mesh):
    n = mesh.shape["tile"]

    def shards(habitat, table, source_cell, ground_cell, start_potential):
        _, rows, cols, rhs = start_potential.shape
        halves = rhs // LANES
        width = cols + 2 * PAD
        f32 = jnp.float32
        dma = pltpu.SemaphoreType.DMA
        field = jax.ShapeDtypeStruct(start_potential.shape, f32)
        vmem = pl.BlockSpec(memory_space=pltpu.VMEM)
        hbm = pl.BlockSpec(memory_space=pltpu.HBM)
        potentials, residual, drop = pl.pallas_call(
            functools.partial(kernel, n, rows, cols),
            out_shape=(field, field, jax.ShapeDtypeStruct((halves, LANES), f32)),
            in_specs=[hbm] * 5,
            out_specs=(vmem, vmem, vmem),
            scratch_shapes=[
                pltpu.VMEM((halves, 3 * rows, width, LANES), f32),
                pltpu.VMEM((halves, 2 * rows, width, LANES), f32),
                pltpu.VMEM((halves, 2 * rows - 2, width, LANES), f32),
                pltpu.VMEM((halves, rows, cols, LANES), f32),
                pltpu.VMEM((2 * rows + 1, width, LANES), f32),
                pltpu.VMEM((2 * rows, width, LANES), f32),
                pltpu.VMEM((2 * rows, width, LANES), f32),
                pltpu.VMEM((6, 2 * rows, cols), f32),
                pltpu.VMEM((width, LANES), f32),
                pltpu.VMEM((width, LANES), f32),
                pltpu.VMEM((width, LANES), f32),
                pltpu.VMEM((halves, n, TILE, LANES), f32),
                pltpu.SMEM(table.shape, f32),
                pltpu.VMEM(habitat.shape, jnp.int32),
                pltpu.VMEM((halves, LANES), jnp.int32),
                pltpu.VMEM((halves, LANES), jnp.int32),
                dma((4,)),
                dma((halves,)),
                dma((5,)), dma((5,)),
                dma((halves,)), dma((halves,)),
                dma((halves, 4, rows)), dma((halves, 4, rows)),
                dma((halves, 4, rows - 1)), dma((halves, 4, rows - 1)),
                dma((halves, n)), dma((halves, n)),
            ],
            compiler_params=pltpu.CompilerParams(
                collective_id=0, has_side_effects=True, vmem_limit_bytes=48 * 2**20),
        )(*(pltpu.with_memory_space_constraint(value, pltpu.HBM) for value in (
            table, habitat, source_cell.reshape(halves, LANES),
            ground_cell.reshape(halves, LANES), start_potential)))
        return potentials, residual, drop.reshape(rhs)

    placed = (
        P(("grp", "tile"), None, None),
        P(),
        P("grp"),
        P("grp"),
        P(("grp", "tile"), None, None, None),
    )
    return jax.shard_map(
        shards,
        mesh=mesh,
        in_specs=placed,
        out_specs=(placed[4], placed[4], P("grp")),
        check_vma=False,
    )
```
